16 devices in a mesh: rep: 2 (over y, z), dp: 8 (over x, core).
Axes of the slice: x: 4, y: 2, z: 1, core: 2. Of those that a mesh axis runs over, the one named last changes fastest.
The devices are a block of a 4x4x8 slice.
Arguments:
- x: bfloat16 [16, 2048, 896], P(('rep', 'dp')), parts along dimension 0
- dy: bfloat16 [16, 2048, 896], P(('rep', 'dp')), parts along dimension 0
- w_gate: bfloat16 [2, 896, 2304], replicated
- w_up: bfloat16 [2, 896, 2304], replicated
- w_down: bfloat16 [2, 2304, 896], replicated
- m_w_gate: float32 [2, 896, 2304], replicated
- m_w_up: float32 [2, 896, 2304], replicated
- m_w_down: float32 [2, 2304, 896], replicated
- v_w_gate: float32 [2, 896, 2304], replicated
- v_w_up: float32 [2, 896, 2304], replicated
- v_w_down: float32 [2, 2304, 896], replicated
Outputs:
- output 1: bfloat16 [4, 896, 2304], P('rep'), parts along dimension 0
- output 2: bfloat16 [4, 896, 2304], P('rep'), parts along dimension 0
- output 3: bfloat16 [4, 2304, 896], P('rep'), parts along dimension 0
- output 4: float32 [4, 896, 2304], P('rep'), parts along dimension 0
- output 5: float32 [4, 896, 2304], P('rep'), parts along dimension 0
- output 6: float32 [4, 2304, 896], P('rep'), parts along dimension 0
- output 7: float32 [4, 896, 2304], P('rep'), parts along dimension 0
- output 8: float32 [4, 896, 2304], P('rep'), parts along dimension 0
- output 9: float32 [4, 2304, 896], P('rep'), parts along dimension 0
There are 2 independent parts. The reference program is written for one: setup_inputs(seed, part) draws one part's arguments, and reference() takes and returns one part's arrays. A program takes and returns all parts, laid end to end along the dimension named above; an argument that names none is the same for every part.
All inputs are finite; a program needn't handle non-finite values.
Results may differ from the reference program's by a relative error of at most 0.02.
Values are sent between devices in bfloat16 or wider.
A program may use at most 768 MiB of HBM per device.

```python
import jax
import jax.numpy as jnp
from jax import lax

SEQUENCES = 8
TOKENS = 2048
D = 896
FF = 2304
LAYERS = 2
NAMES = ("w_gate", "w_up", "w_down")
SHAPES = {"w_gate": (LAYERS, D, FF), "w_up": (LAYERS, D, FF), "w_down": (LAYERS, FF, D)}


def bump(key, n, height):
    away = (jnp.arange(n, dtype=jnp.int32) - jax.random.randint(key, (), 0, n, jnp.int32)) % n
    return jnp.where(away < n // 8, height, 1.0)


def together(key, own, strength):
    shared = jax.random.normal(key, own.shape[1:], jnp.float32)
    return (own + strength * shared) * lax.rsqrt(1 + strength * strength)


def setup_inputs(seed: int = 0, part: int = 0) -> dict:
    kx, kdy, ka, kb, kz, kf, kh, kl, *keys = jax.random.split(jax.random.key(seed), 8 + 3 * len(NAMES))
    kx, kdy, ka, kb = (jax.random.fold_in(k, part) for k in (kx, kdy, ka, kb))
    kw, km, kv = (keys[i::3] for i in range(3))
    shape = (SEQUENCES, TOKENS, D)
    much_x, much_dy = jax.random.uniform(kz, (2,), jnp.float32, 0.0, 1.0)
    loud = 2.0 ** jax.random.uniform(jax.random.fold_in(kz, 1), (), jnp.float32, -1.0, 2.0)
    layers = 2.0 ** jax.random.uniform(kl, (LAYERS, 1, 1), jnp.float32, -1.0, 1.0)
    x = together(ka, jax.random.normal(kx, shape, jnp.float32), much_x) * bump(kf, D, 4.0)
    dy = together(kb, jax.random.normal(kdy, shape, jnp.float32), much_dy)
    drawn = {"x": x.astype(jnp.bfloat16), "dy": (loud * dy * (SEQUENCES * TOKENS) ** -0.5).astype(jnp.bfloat16)}
    for key, name in zip(kw, NAMES, strict=True):
        w = jax.random.normal(key, SHAPES[name], jnp.float32) * SHAPES[name][1] ** -0.5
        drawn[name] = (w * {"w_gate": 1.0, "w_up": bump(kh, FF, 4.0), "w_down": layers}[name]).astype(jnp.bfloat16)
    for key, name in zip(km, NAMES, strict=True):
        drawn[f"m_{name}"] = 0.1 * jax.random.normal(key, SHAPES[name], jnp.float32)
    for key, name in zip(kv, NAMES, strict=True):
        drawn[f"v_{name}"] = jax.random.uniform(key, SHAPES[name], jnp.float32, 0.005, 0.015)
    return drawn


def matmul(a, w):
    return jnp.dot(a, w, preferred_element_type=jnp.float32).astype(jnp.bfloat16)


def normed(h):
    wide = h.astype(jnp.float32)
    scale = lax.rsqrt(jnp.mean(wide**2, -1, keepdims=True) + 1e-6)
    return (wide * scale).astype(jnp.bfloat16)


def layer(h, w):
    a = normed(h)
    gate = jnp.dot(a, w["w_gate"], preferred_element_type=jnp.float32)
    up = jnp.dot(a, w["w_up"], preferred_element_type=jnp.float32)
    return h + matmul((jax.nn.silu(gate) * up).astype(jnp.bfloat16), w["w_down"])


def adamw(w, m, v, g):
    m = 0.9 * m + 0.1 * g
    v = 0.95 * v + 0.05 * g * g
    step = m * lax.rsqrt(v + 1e-8) + 0.1 * w
    return (w - 0.02 * step).astype(jnp.bfloat16), m, v


def stack(weights, h):
    return lax.scan(lambda h, w: (layer(h, w), None), h, weights)[0]


def reference(x, dy, w_gate, w_up, w_down, m_w_gate, m_w_up, m_w_down, v_w_gate, v_w_up, v_w_down):
    weights = dict(zip(NAMES, (w_gate, w_up, w_down), strict=True))

    def take(so_far, sequence):
        h, by_y = sequence
        _, back = jax.vjp(lambda w: stack(w, h), weights)
        return jax.tree.map(lambda total, term: total + term.astype(jnp.float32), so_far, back(by_y)[0]), None

    none_yet = {name: jnp.zeros(w.shape, jnp.float32) for name, w in weights.items()}
    by_weights, _ = lax.scan(take, none_yet, (x, dy))
    gradients = [by_weights[name].astype(jnp.bfloat16).astype(jnp.float32) for name in NAMES]
    new = [
        adamw(w.astype(jnp.float32), m, v, g)
        for w, m, v, g in zip((w_gate, w_up, w_down), (m_w_gate, m_w_up, m_w_down), (v_w_gate, v_w_up, v_w_down), gradients, strict=True)
    ]
    return tuple(one[which] for which in range(3) for one in new)
```

```python
import functools

import jax
import jax.numpy as jnp
from jax import lax
from jax.experimental import pallas as pl
from jax.experimental.pallas import tpu as pltpu
from jax.sharding import PartitionSpec as P


F32, BF16 = jnp.float32, jnp.bfloat16
PARAMS = functools.partial(pltpu.CompilerParams, vmem_limit_bytes=60 * 2**20)


def mm(a, b, ca=1, cb=0):
    return lax.dot_general(a, b, (((ca,), (cb,)), ((), ())), preferred_element_type=F32)


def normed(wide):
    scale = lax.rsqrt(jnp.mean(wide * wide, -1, keepdims=True) + 1e-6)
    return (wide * scale).astype(BF16)


def sigmoid(x):
    return 0.5 * jnp.tanh(0.5 * x) + 0.5


def cost(flops, nbytes):
    return pl.CostEstimate(flops=int(flops), bytes_accessed=int(nbytes), transcendentals=0)


def whole(shape):
    return pl.BlockSpec(shape, lambda *_: (0,) * len(shape), pipeline_mode=pl.Buffered(1))


def layer_of(array, number):
    return pl.BlockSpec((None, *array.shape[1:]), lambda *_: (number, 0, 0), pipeline_mode=pl.Buffered(1))


def chunks(ff, width):
    return [slice(i, i + width) for i in range(0, ff, width)]


def forward_kernel(width, h_ref, wg_ref, wu_ref, wd_ref, o_ref, hid_ref):
    wide = h_ref[...].astype(F32)
    a = normed(wide)
    for c in chunks(wg_ref.shape[1], width):
        gate, up = mm(a, wg_ref[:, c]), mm(a, wu_ref[:, c])
        hid_ref[:, c] = (gate * sigmoid(gate) * up).astype(BF16)
    y = mm(hid_ref[...], wd_ref[...]).astype(BF16).astype(F32)
    o_ref[...] = (wide + y).astype(BF16)


def forward(number, h, wg, wu, wd, tile=512, width=768):
    tokens, d = h.shape
    ff = wg.shape[2]
    return pl.pallas_call(
        functools.partial(forward_kernel, width),
        name="forward",
        grid=(tokens // tile,),
        in_specs=[pl.BlockSpec((tile, d), lambda i: (i, 0)), layer_of(wg, number), layer_of(wu, number), layer_of(wd, number)],
        out_specs=pl.BlockSpec((tile, d), lambda i: (i, 0)),
        out_shape=jax.ShapeDtypeStruct((tokens, d), BF16),
        scratch_shapes=[pltpu.VMEM((tile, ff), BF16)],
        compiler_params=PARAMS(),
        cost_estimate=cost(6 * tokens * d * ff, 2 * (2 * tokens * d + 3 * d * ff)),
    )(h, wg, wu, wd)


PAIRED, PASSED, ARRIVED = 2, 4, 6


def gradients_kernel(size, tile, h_ref, dy_ref, wg_ref, wu_ref, wd_ref, o_ref, *refs):
    *kept, a, x, y, g, pr, p, r1a, r1b, r2a, r2b, send, recv = refs
    step = pl.program_id(0)
    steps = pl.num_programs(0) - ARRIVED // 3
    pieces = 3 * steps
    slots = g.shape[0]
    rows = g.shape[1] // size
    width = g.shape[2]
    a_half, b_half = pl.ds(0, width // 2), pl.ds(width // 2, width // 2)
    quarters = size // 2
    me = lax.axis_index("dp")
    core, chip = lax.rem(me, 2), me // 2
    partner = me + 1 - 2 * core
    right, left = lax.rem(me + 2, size), lax.rem(me + size - 2, size)

    def of_chip(offset):
        return pl.ds(pl.multiple_of(lax.rem(chip + offset, quarters) * rows, 16), rows)

    def half(which):
        return pl.ds(pl.multiple_of(which * quarters * rows, 16), quarters * rows)

    def copy(kind, j, source, target, device):
        return pltpu.make_async_remote_copy(
            src_ref=source,
            dst_ref=target.at[j],
            send_sem=send.at[kind, j],
            recv_sem=recv.at[kind, j],
            device_id={"dp": device},
            device_id_type=pl.DeviceIdType.MESH,
        )

    def to_partner(j):
        return copy(0, j, g.at[lax.rem(j, slots), half(1 - core)], pr, partner)

    def first(j):
        opposite = of_chip(2)
        return copy(1, j, p.at[j, opposite, a_half], r1a, right), copy(2, j, p.at[j, opposite, b_half], r1b, left)

    def second(j):
        return copy(3, j, p.at[j, of_chip(1)], r2a, right), copy(4, j, p.at[j, of_chip(quarters - 1)], r2b, left)

    @pl.when(step == 0)
    def _():
        barrier = pltpu.get_barrier_semaphore()
        for device in (partner, left, right):
            pl.semaphore_signal(barrier, inc=1, device_id={"dp": device}, device_id_type=pl.DeviceIdType.MESH)
        pl.semaphore_wait(barrier, 3)
        for i in range(0, a.shape[0], tile):
            part = normed(h_ref[i : i + tile].astype(F32))
            a[i : i + tile] = part
            x[0, :, i : i + tile] = dy_ref[i : i + tile].T
            x[1, :, i : i + tile] = part.T

    @pl.when(step < steps)
    def _():
        for i in range(0, a.shape[0], tile):
            t = slice(i, i + tile)
            gate, up = mm(a[t], wg_ref[...]), mm(a[t], wu_ref[...])
            by_hid = mm(dy_ref[t], wd_ref[...], 1, 1).astype(BF16).astype(F32)
            s = sigmoid(gate)
            silu = gate * s
            y[0, t] = (silu * up).astype(BF16)
            dg = (by_hid * up * (s + silu * (1.0 - s))).astype(BF16)
            du = (by_hid * silu).astype(BF16)
            y[1, t] = dg
            y[2, t] = du
            if kept:
                kept[0][0, t] = dg
                kept[0][1, t] = du

    @pl.loop(0, 3)
    def _(which):
        k = 3 * step + which

        def stage(after):
            return pl.when((k >= after) & (k < pieces + after))

        @stage(0)
        def _():
            g[lax.rem(k, slots)] = mm(x[jnp.minimum(which, 1)], y[which]).astype(BF16)

        @stage(PAIRED)
        def _():
            j = k - PAIRED
            to_partner(j).wait()
            p[j] = (g[lax.rem(j, slots), half(core)].astype(F32) + pr[j].astype(F32)).astype(BF16)

        @stage(PASSED)
        def _():
            j = k - PASSED
            for one in first(j):
                one.wait()
            p[j, of_chip(1), a_half] = (p[j, of_chip(1), a_half].astype(F32) + r1a[j].astype(F32)).astype(BF16)
            p[j, of_chip(quarters - 1), b_half] = (p[j, of_chip(quarters - 1), b_half].astype(F32) + r1b[j].astype(F32)).astype(BF16)

        @stage(ARRIVED)
        def _():
            j = k - ARRIVED
            for one in second(j):
                one.wait()
            total = (p[j, of_chip(0)].astype(F32) + r2a[j].astype(F32) + r2b[j].astype(F32)).astype(BF16)
            o_ref[lax.rem(j, 3), :, pl.ds(pl.multiple_of((j // 3) * width, 128), width)] = total

        @stage(PASSED)
        def _():
            for one in second(k - PASSED):
                one.start()

        @stage(PAIRED)
        def _():
            for one in first(k - PAIRED):
                one.start()

        @stage(0)
        def _():
            to_partner(k).start()


def gradients(size, number, h, dy, wg, wu, wd, keep, width=256, tile=512):
    tokens, d = h.shape
    ff = wg.shape[2]
    steps, rows, half = ff // width, d // size, d // 2
    pieces = 3 * steps

    def now(k):
        return jnp.minimum(k, steps - 1)

    column = pl.BlockSpec((None, d, width), lambda k: (number, 0, now(k)))
    out_specs, out_shape = [whole((3, rows, ff))], [jax.ShapeDtypeStruct((3, rows, ff), BF16)]
    if keep:
        out_specs += [pl.BlockSpec((2, tokens, width), lambda k: (0, 0, now(k)))]
        out_shape += [jax.ShapeDtypeStruct((2, tokens, ff), BF16)]
    return pl.pallas_call(
        functools.partial(gradients_kernel, size, tile),
        name="gradients",
        grid=(steps + ARRIVED // 3,),
        in_specs=[whole((tokens, d))] * 2 + [column, column, pl.BlockSpec((None, width, d), lambda k: (number, now(k), 0))],
        out_specs=out_specs,
        out_shape=out_shape,
        scratch_shapes=[
            pltpu.VMEM((tokens, d), BF16),
            pltpu.VMEM((2, d, tokens), BF16),
            pltpu.VMEM((3, tokens, width), BF16),
            pltpu.VMEM((PAIRED + 1, d, width), BF16),
            pltpu.VMEM((pieces, half, width), BF16),
            pltpu.VMEM((pieces, half, width), BF16),
            pltpu.VMEM((pieces, rows, width // 2), BF16),
            pltpu.VMEM((pieces, rows, width // 2), BF16),
            pltpu.VMEM((pieces, rows, width), BF16),
            pltpu.VMEM((pieces, rows, width), BF16),
            pltpu.SemaphoreType.DMA((5, pieces)),
            pltpu.SemaphoreType.DMA((5, pieces)),
        ],
        compiler_params=PARAMS(collective_id=number, has_side_effects=True),
        cost_estimate=cost(18 * tokens * d * ff, 2 * (2 * tokens * d + 2 * tokens * ff + 6 * d * ff)),
    )(h, dy, wg, wu, wd)


def back_kernel(h_ref, dy_ref, dg_ref, du_ref, wg_ref, wu_ref, o_ref):
    by_a = mm(dg_ref[...], wg_ref[...], 1, 1).astype(BF16).astype(F32)
    by_a = (by_a + mm(du_ref[...], wu_ref[...], 1, 1).astype(BF16).astype(F32)).astype(BF16).astype(F32)
    wide = h_ref[...].astype(F32)
    scale = lax.rsqrt(jnp.mean(wide * wide, -1, keepdims=True) + 1e-6)
    by_h = scale * by_a - wide * (scale * scale * scale * jnp.mean(by_a * wide, -1, keepdims=True))
    o_ref[...] = (dy_ref[...].astype(F32) + by_h.astype(BF16).astype(F32)).astype(BF16)


def back(number, h, dy, y, wg, wu, tile=512):
    tokens, d = h.shape
    ff = wg.shape[2]
    row = pl.BlockSpec((tile, d), lambda i: (i, 0))
    by_gate, by_up = (pl.BlockSpec((None, tile, ff), lambda i, which=which: (which, i, 0)) for which in (0, 1))
    return pl.pallas_call(
        back_kernel,
        name="back",
        grid=(tokens // tile,),
        in_specs=[row, row, by_gate, by_up, layer_of(wg, number), layer_of(wu, number)],
        out_specs=row,
        out_shape=jax.ShapeDtypeStruct((tokens, d), BF16),
        compiler_params=PARAMS(),
        cost_estimate=cost(4 * tokens * d * ff, 2 * (3 * tokens * d + 2 * d * ff + 2 * tokens * ff)),
    )(h, dy, y, y, wg, wu)


def adamw_step(g, w_ref, m_ref, v_ref, ow_ref, om_ref, ov_ref):
    g = g.astype(F32)
    m = 0.9 * m_ref[...] + 0.1 * g
    v = 0.95 * v_ref[...] + 0.05 * g * g
    w = w_ref[...].astype(F32)
    ow_ref[...] = (w - 0.02 * (m * lax.rsqrt(v + 1e-8) + 0.1 * w)).astype(BF16)
    om_ref[...] = m
    ov_ref[...] = v


def adamw_kernel(place_ref, w_ref, m_ref, v_ref, *refs):
    parts, outs = refs[:10], refs[-3:]
    for which in range(8):

        @pl.when(pl.program_id(0) == which)
        def _(which=which):
            group = parts[5 * (which // 4) :]
            at = which % 4
            g = group[at][...] if at < 3 else jnp.concatenate([group[3][...], group[4][...]], 1)
            adamw_step(g, w_ref, m_ref, v_ref, *outs)


def adamw_turned_kernel(place_ref, w_ref, m_ref, v_ref, *refs):
    parts, outs, g_ref = refs[:10], refs[-4:-1], refs[-1]
    rows = parts[0].shape[0]
    early = pl.program_id(0) < pl.num_programs(0) // 2

    def put(which, value):
        g_ref[pl.ds(pl.multiple_of(place_ref[which] * rows, 16), rows)] = value

    for which in range(8):
        group = parts[5 * (which // 4) :]
        at = which % 4
        if at < 3:
            put(which, group[at][...])
        else:
            put(which, jnp.where(early, group[3][...], group[4][...]))
    adamw_step(g_ref[...].T, w_ref, m_ref, v_ref, *outs)


def adamw(place, number, at, parts, w, m, v, turned, so_far, width=384):
    rows, ff = parts[0].shape[1:]
    d = rows * place.shape[0]
    so_far = so_far or ()
    if turned:
        steps, kernel = ff // width, adamw_turned_kernel
        per = steps // 2
        big = pl.BlockSpec((None, width, d), lambda i, place: (number, i, 0))
        three = [pl.BlockSpec((None, rows, width), lambda i, place: (at, 0, i))] * 3
        three += [pl.BlockSpec((None, rows, width), lambda i, place: (at, 0, jnp.minimum(i, per - 1)))]
        three += [pl.BlockSpec((None, rows, width), lambda i, place: (at, 0, jnp.maximum(i - per, 0)))]
        scratch = [pltpu.VMEM((d, width), BF16)]
    else:
        steps, kernel = place.shape[0], adamw_kernel
        big = pl.BlockSpec((None, rows, ff), lambda i, place: (number, place[i], 0))
        three = [pl.BlockSpec((None, *part.shape[1:]), lambda i, place: (at, 0, 0), pipeline_mode=pl.Buffered(1)) for part in parts[:5]]
        scratch = []
    return pl.pallas_call(
        kernel,
        name="adamw",
        grid_spec=pltpu.PrefetchScalarGridSpec(
            num_scalar_prefetch=1,
            grid=(steps,),
            in_specs=[big, big, big, *three, *three, *[pl.BlockSpec(memory_space=pl.ANY)] * len(so_far)],
            out_specs=[big] * 3,
            scratch_shapes=scratch,
        ),
        out_shape=[jax.ShapeDtypeStruct(w.shape, BF16), jax.ShapeDtypeStruct(m.shape, F32), jax.ShapeDtypeStruct(v.shape, F32)],
        input_output_aliases={14 + i: i for i in range(len(so_far))},
        compiler_params=PARAMS(),
        cost_estimate=cost(5 * 2048 * d * ff // 2, 22 * d * ff),
    )(place, w, m, v, *parts, *so_far)


def solution(mesh):
    size = mesh.shape["dp"]
    swap = [(i, i ^ 1) for i in range(size)]
    to_right = [(i, (i + 2) % size) for i in range(size)]
    to_left = [(i, (i - 2) % size) for i in range(size)]

    def step(x, dy, *arrays):
        weights, moments, squares = (arrays[i : i + 3] for i in (0, 3, 6))
        layers = weights[0].shape[0]
        me = lax.axis_index("dp")
        core, chip = me % 2, me // 2
        offsets = jnp.array([0, size // 2 - 1, 1, 2], jnp.int32)
        place = ((chip + offsets) % (size // 2))[None] + jnp.stack([core, 1 - core])[:, None] * (size // 2)
        place = place.reshape(-1).astype(jnp.int32)

        def hop(one, to):
            return lax.ppermute(one, "dp", to)

        def gathered(own):
            middle = own.shape[2] // 2
            left, right = hop(own, to_right), hop(own, to_left)
            first = hop(left[:, :, :middle], to_right)
            second = hop(right[:, :, middle:], to_left)
            pairs = [hop(own, swap), hop(left, swap), hop(right, swap)]
            pairs += [hop(first, swap), hop(second, swap)]
            return (own, left, right, first, second, *pairs)

        h, kept = x[0], []
        for number in range(layers):
            kept.append(h)
            if number < layers - 1:
                h = forward(number, h, *weights)
        by_h, out, sums = dy[0], [None] * 3, []
        for number in reversed(range(layers)):
            own, *by_both = gradients(size, number, kept[number], by_h, *weights, number > 0)
            parts = gathered(own)
            for at, which in enumerate((2, 0, 1)):
                sums.append((number, which, at, parts))
            if number:
                by_h = back(number, kept[number], by_h, by_both[0], *weights[:2])
        for number, which, at, parts in sums:
            out[which] = adamw(place, number, at, parts, weights[which], moments[which], squares[which], which == 2, out[which])
        return tuple(one[which] for which in range(3) for one in out)

    return jax.shard_map(
        step,
        mesh=mesh,
        in_specs=(P(("rep", "dp"), None, None),) * 2 + (P(None, None, None),) * 9,
        out_specs=(P("rep", None, None),) * 9,
        check_vma=False,
    )
```

```python
import functools

import jax
import jax.numpy as jnp
from jax import lax
from jax.experimental import pallas as pl
from jax.experimental.pallas import tpu as pltpu
from jax.sharding import PartitionSpec as P


F32, BF16 = jnp.float32, jnp.bfloat16
PARAMS = functools.partial(pltpu.CompilerParams, vmem_limit_bytes=60 * 2**20)


def mm(a, b, ca=1, cb=0):
    return lax.dot_general(a, b, (((ca,), (cb,)), ((), ())), preferred_element_type=F32)


def normed(wide):
    scale = lax.rsqrt(jnp.mean(wide * wide, -1, keepdims=True) + 1e-6)
    return (wide * scale).astype(BF16)


def sigmoid(x):
    return 0.5 * jnp.tanh(0.5 * x) + 0.5


def cost(flops, nbytes):
    return pl.CostEstimate(flops=int(flops), bytes_accessed=int(nbytes), transcendentals=0)


def whole(shape):
    return pl.BlockSpec(shape, lambda *_: (0,) * len(shape), pipeline_mode=pl.Buffered(1))


def layer_of(array, number):
    return pl.BlockSpec((None, *array.shape[1:]), lambda *_: (number, 0, 0), pipeline_mode=pl.Buffered(1))


def chunks(ff, width):
    return [slice(i, i + width) for i in range(0, ff, width)]


def forward_kernel(width, h_ref, wg_ref, wu_ref, wd_ref, o_ref, gate_ref, up_ref, hid_ref):
    wide = h_ref[...].astype(F32)
    a = normed(wide)
    for c in chunks(wg_ref.shape[1], width):
        gate, up = mm(a, wg_ref[:, c]), mm(a, wu_ref[:, c])
        gate_ref[:, c], up_ref[:, c] = gate, up
        hid_ref[:, c] = (gate * sigmoid(gate) * up).astype(BF16)
    y = mm(hid_ref[...], wd_ref[...]).astype(BF16).astype(F32)
    o_ref[...] = (wide + y).astype(BF16)


def forward(number, h, wg, wu, wd, tile=256, width=768):
    tokens, d = h.shape
    ff = wg.shape[2]
    return pl.pallas_call(
        functools.partial(forward_kernel, width),
        name="forward",
        grid=(tokens // tile,),
        in_specs=[pl.BlockSpec((tile, d), lambda i: (i, 0)), layer_of(wg, number), layer_of(wu, number), layer_of(wd, number)],
        out_specs=[pl.BlockSpec((tile, width), lambda i: (i, 0)) for width in (d, ff, ff)],
        out_shape=[jax.ShapeDtypeStruct((tokens, d), BF16)] + [jax.ShapeDtypeStruct((tokens, ff), F32)] * 2,
        scratch_shapes=[pltpu.VMEM((tile, ff), BF16)],
        compiler_params=PARAMS(),
        cost_estimate=cost(6 * tokens * d * ff, 2 * (2 * tokens * d + 3 * d * ff + 4 * tokens * ff)),
    )(h, wg, wu, wd)


PAIRED, PASSED, ARRIVED = 3, 6, 9


def gradients_kernel(size, tile, known, h_ref, dy_ref, gate_ref, up_ref, wd_ref, o_ref, *refs):
    *kept, x, y, g, pr, p, r1a, r1b, r2a, r2b, send, recv = refs
    tokens = h_ref.shape[0]
    if not known:
        *kept, a = kept
    step = pl.program_id(0)
    steps = pl.num_programs(0) - ARRIVED // 3
    pieces = 3 * steps
    slots = g.shape[0]
    rows = g.shape[1] // size
    width = g.shape[2]
    a_half, b_half = pl.ds(0, width // 2), pl.ds(width // 2, width // 2)
    quarters = size // 2
    me = lax.axis_index("dp")
    core, chip = lax.rem(me, 2), me // 2
    partner = me + 1 - 2 * core
    right, left = lax.rem(me + 2, size), lax.rem(me + size - 2, size)

    def of_chip(offset):
        return pl.ds(pl.multiple_of(lax.rem(chip + offset, quarters) * rows, 16), rows)

    def half(which):
        return pl.ds(pl.multiple_of(which * quarters * rows, 16), quarters * rows)

    def copy(kind, j, source, target, device):
        return pltpu.make_async_remote_copy(
            src_ref=source,
            dst_ref=target.at[j],
            send_sem=send.at[kind, j],
            recv_sem=recv.at[kind, j],
            device_id={"dp": device},
            device_id_type=pl.DeviceIdType.MESH,
        )

    def to_partner(j):
        return copy(0, j, g.at[lax.rem(j, slots), half(1 - core)], pr, partner)

    def first(j):
        opposite = of_chip(2)
        return copy(1, j, p.at[j, opposite, a_half], r1a, right), copy(2, j, p.at[j, opposite, b_half], r1b, left)

    def second(j):
        return copy(3, j, p.at[j, of_chip(1)], r2a, right), copy(4, j, p.at[j, of_chip(quarters - 1)], r2b, left)

    @pl.when(step == 0)
    def _():
        barrier = pltpu.get_barrier_semaphore()
        for device in (partner, left, right):
            pl.semaphore_signal(barrier, inc=1, device_id={"dp": device}, device_id_type=pl.DeviceIdType.MESH)
        pl.semaphore_wait(barrier, 3)
        for i in range(0, tokens, tile):
            part = normed(h_ref[i : i + tile].astype(F32))
            if not known:
                a[i : i + tile] = part
            x[0, :, i : i + tile] = dy_ref[i : i + tile].T
            x[1, :, i : i + tile] = part.T

    @pl.when(step < steps)
    def _():
        for i in range(0, tokens, tile):
            t = slice(i, i + tile)
            gate, up = (gate_ref[t], up_ref[t]) if known else (mm(a[t], gate_ref[...]), mm(a[t], up_ref[...]))
            by_hid = mm(dy_ref[t], wd_ref[...], 1, 1).astype(BF16).astype(F32)
            s = sigmoid(gate)
            silu = gate * s
            y[0, t] = (silu * up).astype(BF16)
            dg = (by_hid * up * (s + silu * (1.0 - s))).astype(BF16)
            du = (by_hid * silu).astype(BF16)
            y[1, t] = dg
            y[2, t] = du
            if kept:
                kept[0][0, t] = dg
                kept[0][1, t] = du

    @pl.loop(0, 3)
    def _(which):
        k = 3 * step + which

        def stage(after):
            return pl.when((k >= after) & (k < pieces + after))

        @stage(0)
        def _():
            g[lax.rem(k, slots)] = mm(x[jnp.minimum(which, 1)], y[which]).astype(BF16)

        @stage(PAIRED)
        def _():
            j = k - PAIRED
            to_partner(j).wait()
            p[j] = (g[lax.rem(j, slots), half(core)].astype(F32) + pr[j].astype(F32)).astype(BF16)

        @stage(PASSED)
        def _():
            j = k - PASSED
            for one in first(j):
                one.wait()
            p[j, of_chip(1), a_half] = (p[j, of_chip(1), a_half].astype(F32) + r1a[j].astype(F32)).astype(BF16)
            p[j, of_chip(quarters - 1), b_half] = (p[j, of_chip(quarters - 1), b_half].astype(F32) + r1b[j].astype(F32)).astype(BF16)

        @stage(ARRIVED)
        def _():
            j = k - ARRIVED
            for one in second(j):
                one.wait()
            total = (p[j, of_chip(0)].astype(F32) + r2a[j].astype(F32) + r2b[j].astype(F32)).astype(BF16)
            o_ref[lax.rem(j + 2, 3), :, pl.ds(pl.multiple_of((j // 3) * width, 128), width)] = total

        @stage(PASSED)
        def _():
            for one in second(k - PASSED):
                one.start()

        @stage(PAIRED)
        def _():
            for one in first(k - PAIRED):
                one.start()

        @stage(0)
        def _():
            to_partner(k).start()


def gradients(size, number, h, dy, known, wg, wu, wd, keep, width=256, tile=512):
    tokens, d = h.shape
    ff = wg.shape[2]
    steps, rows, half = ff // width, d // size, d // 2
    pieces = 3 * steps

    def now(k):
        return jnp.minimum(k, steps - 1)

    if known:
        column, pair = pl.BlockSpec((tokens, width), lambda k: (0, now(k))), known
    else:
        column, pair = pl.BlockSpec((None, d, width), lambda k: (number, 0, now(k))), (wg, wu)
    out_specs, out_shape = [whole((3, rows, ff))], [jax.ShapeDtypeStruct((3, rows, ff), BF16)]
    if keep:
        out_specs += [pl.BlockSpec((2, tokens, width), lambda k: (0, 0, now(k)))]
        out_shape += [jax.ShapeDtypeStruct((2, tokens, ff), BF16)]
    return pl.pallas_call(
        functools.partial(gradients_kernel, size, tile, bool(known)),
        name="gradients",
        grid=(steps + ARRIVED // 3,),
        in_specs=[whole((tokens, d))] * 2 + [column, column, pl.BlockSpec((None, width, d), lambda k: (number, now(k), 0))],
        out_specs=out_specs,
        out_shape=out_shape,
        scratch_shapes=[
            *([] if known else [pltpu.VMEM((tokens, d), BF16)]),
            pltpu.VMEM((2, d, tokens), BF16),
            pltpu.VMEM((3, tokens, width), BF16),
            pltpu.VMEM((PAIRED + 1, d, width), BF16),
            pltpu.VMEM((pieces, half, width), BF16),
            pltpu.VMEM((pieces, half, width), BF16),
            pltpu.VMEM((pieces, rows, width // 2), BF16),
            pltpu.VMEM((pieces, rows, width // 2), BF16),
            pltpu.VMEM((pieces, rows, width), BF16),
            pltpu.VMEM((pieces, rows, width), BF16),
            pltpu.SemaphoreType.DMA((5, pieces)),
            pltpu.SemaphoreType.DMA((5, pieces)),
        ],
        compiler_params=PARAMS(collective_id=number, has_side_effects=True),
        cost_estimate=cost((8 if known else 12) * tokens * d * ff, 2 * (2 * tokens * d + 2 * tokens * ff + 6 * d * ff)),
    )(h, dy, *pair, wd)


def back_kernel(h_ref, dy_ref, dg_ref, du_ref, wg_ref, wu_ref, o_ref):
    by_a = mm(dg_ref[...], wg_ref[...], 1, 1).astype(BF16).astype(F32)
    by_a = (by_a + mm(du_ref[...], wu_ref[...], 1, 1).astype(BF16).astype(F32)).astype(BF16).astype(F32)
    wide = h_ref[...].astype(F32)
    scale = lax.rsqrt(jnp.mean(wide * wide, -1, keepdims=True) + 1e-6)
    by_h = scale * by_a - wide * (scale * scale * scale * jnp.mean(by_a * wide, -1, keepdims=True))
    o_ref[...] = (dy_ref[...].astype(F32) + by_h.astype(BF16).astype(F32)).astype(BF16)


def back(number, h, dy, y, wg, wu, tile=512):
    tokens, d = h.shape
    ff = wg.shape[2]
    row = pl.BlockSpec((tile, d), lambda i: (i, 0))
    by_gate, by_up = (pl.BlockSpec((None, tile, ff), lambda i, which=which: (which, i, 0)) for which in (0, 1))
    return pl.pallas_call(
        back_kernel,
        name="back",
        grid=(tokens // tile,),
        in_specs=[row, row, by_gate, by_up, layer_of(wg, number), layer_of(wu, number)],
        out_specs=row,
        out_shape=jax.ShapeDtypeStruct((tokens, d), BF16),
        compiler_params=PARAMS(),
        cost_estimate=cost(4 * tokens * d * ff, 2 * (3 * tokens * d + 2 * d * ff + 2 * tokens * ff)),
    )(h, dy, y, y, wg, wu)


FLIGHT = 3


def adamw_kernel(number, first, count, blocks, size, turned, aliased, *refs):
    parts, refs = refs[:10], refs[10:]
    sources, refs = refs[: 3 * count], refs[3 * count + aliased :]
    targets, refs = refs[: 3 * count], refs[3 * count :]
    g_buf, wi, mi, vi, wo, mo, vo, g_sem, in_sem, out_sem = refs
    rows, per = wi.shape[1], blocks // count
    shard, middle = parts[0].shape[1], parts[3].shape[2]
    quarters = size // 2
    me = lax.axis_index("dp")
    core, chip = lax.rem(me, 2), me // 2

    def place(which):
        at = lax.rem(which, 4)
        offset = jnp.where(at == 1, quarters - 1, jnp.where(at == 2, 1, jnp.where(at == 3, 2, 0)))
        side = jnp.where(which < 4, core, 1 - core)
        return side * quarters + lax.rem(chip + offset, quarters)

    def of_shard(which, matrix, target, sem):
        group, at = parts[5 * (which // 4) :], which % 4
        if at < 3:
            return [pltpu.make_async_copy(group[at].at[matrix], target, sem)]
        return [
            pltpu.make_async_copy(group[3].at[matrix], target.at[:, pl.ds(0, middle)], sem),
            pltpu.make_async_copy(group[4].at[matrix], target.at[:, pl.ds(middle, middle)], sem),
        ]

    def move(c, arrays, buffers, sem, into):
        slot, block = lax.rem(c, FLIGHT), lax.rem(c, per)
        start = block if turned else place(block)
        here = pl.ds(pl.multiple_of(start * rows, 16), rows)
        for matrix in range(count):

            @pl.when(c // per == matrix)
            def _(matrix=matrix):
                for kind in range(3):
                    far, near = arrays[kind * count + matrix].at[number, here], buffers[kind].at[slot]
                    pltpu.make_async_copy(*((far, near) if into else (near, far)), sem.at[kind, slot]).start()

                if into and not turned:
                    for which in range(8):

                        @pl.when(block == which)
                        def _(which=which):
                            for one in of_shard(which, first + matrix, g_buf.at[slot], g_sem.at[slot]):
                                one.start()

    def settle(c, arrays, buffers, sem, into):
        slot = lax.rem(c, FLIGHT)
        for kind in range(3):
            far, near = arrays[kind * count].at[number, pl.ds(0, rows)], buffers[kind].at[slot]
            pltpu.make_async_copy(*((far, near) if into else (near, far)), sem.at[kind, slot]).wait()
        if into and not turned:
            pltpu.make_async_copy(parts[0].at[first], g_buf.at[slot], g_sem.at[slot]).wait()

    def fetch(c):
        move(c, sources, (wi, mi, vi), in_sem, True)

    if turned:
        for which in range(8):
            for one in of_shard(which, first, g_buf.at[pl.ds(pl.multiple_of(place(which) * shard, 16), shard)], g_sem.at[which]):
                one.start()
    for c in range(FLIGHT):
        fetch(c)
    if turned:
        for which in range(8):
            pltpu.make_async_copy(parts[0].at[first], g_buf.at[pl.ds(0, shard)], g_sem.at[which]).wait()

    @pl.loop(0, blocks)
    def _(c):
        slot = lax.rem(c, FLIGHT)
        settle(c, sources, (wi, mi, vi), in_sem, True)

        @pl.when(c >= FLIGHT)
        def _():
            settle(c - FLIGHT, targets, (wo, mo, vo), out_sem, False)

        g = g_buf[:, pl.ds(pl.multiple_of(c * rows, 128), rows)].T if turned else g_buf[slot]
        g = g.astype(F32)
        m = 0.9 * mi[slot] + 0.1 * g
        v = 0.95 * vi[slot] + 0.05 * g * g
        w = wi[slot].astype(F32)
        wo[slot] = (w - 0.02 * (m * lax.rsqrt(v + 1e-8) + 0.1 * w)).astype(BF16)
        mo[slot] = m
        vo[slot] = v
        move(c, targets, (wo, mo, vo), out_sem, False)

        @pl.when(c + FLIGHT < blocks)
        def _():
            fetch(c + FLIGHT)

    for c in range(blocks - FLIGHT, blocks):
        settle(c, targets, (wo, mo, vo), out_sem, False)


def adamw(size, number, first, parts, weights, moments, squares, turned, so_far, width=256):
    count = len(weights)
    shard, ff = parts[0].shape[1:]
    d = shard * size
    so_far = so_far or ()
    rows, columns = (width, d) if turned else (shard, ff)
    blocks = count * weights[0].shape[1] // rows
    hbm = pl.BlockSpec(memory_space=pl.ANY)
    inputs = (*parts, *weights, *moments, *squares, *so_far)
    return pl.pallas_call(
        functools.partial(adamw_kernel, number, first, count, blocks, size, turned, len(so_far)),
        name="adamw",
        in_specs=[hbm] * len(inputs),
        out_specs=[hbm] * (3 * count),
        out_shape=[jax.ShapeDtypeStruct(one.shape, one.dtype) for one in (*weights, *moments, *squares)],
        scratch_shapes=[
            pltpu.VMEM((d, ff) if turned else (FLIGHT, rows, columns), BF16),
            *[pltpu.VMEM((FLIGHT, rows, columns), dtype) for dtype in (BF16, F32, F32) * 2],
            pltpu.SemaphoreType.DMA((8,) if turned else (FLIGHT,)),
            pltpu.SemaphoreType.DMA((3, FLIGHT)),
            pltpu.SemaphoreType.DMA((3, FLIGHT)),
        ],
        input_output_aliases={10 + 3 * count + i: i for i in range(len(so_far))},
        compiler_params=PARAMS(),
        cost_estimate=cost(count * 5 * 2048 * d * ff // 2, count * 22 * d * ff),
    )(*inputs)


def solution(mesh):
    size = mesh.shape["dp"]
    swap = [(i, i ^ 1) for i in range(size)]
    to_right = [(i, (i + 2) % size) for i in range(size)]
    to_left = [(i, (i - 2) % size) for i in range(size)]

    def step(x, dy, *arrays):
        weights, moments, squares = (arrays[i : i + 3] for i in (0, 3, 6))
        layers = weights[0].shape[0]

        def hop(one, to):
            return lax.ppermute(one, "dp", to)

        def gathered(own):
            middle = own.shape[2] // 2
            left, right = hop(own, to_right), hop(own, to_left)
            first = hop(left[:, :, :middle], to_right)
            second = hop(right[:, :, middle:], to_left)
            pairs = [hop(own, swap), hop(left, swap), hop(right, swap)]
            pairs += [hop(first, swap), hop(second, swap)]
            return (own, left, right, first, second, *pairs)

        h, kept, known = x[0], [], []
        for number in range(layers):
            kept.append(h)
            both = ()
            if number < layers - 1:
                h, *both = forward(number, h, *weights)
            known.append(both)
        by_h, every = dy[0], []
        for number in reversed(range(layers)):
            own, *by_both = gradients(size, number, kept[number], by_h, known[number], *weights, number > 0)
            every.append((number, gathered(own)))
            if number:
                by_h = back(number, kept[number], by_h, by_both[0], *weights[:2])
        side, down = None, None
        for number, parts in every:
            side = adamw(size, number, 0, parts, weights[:2], moments[:2], squares[:2], False, side)
            down = adamw(size, number, 2, parts, weights[2:], moments[2:], squares[2:], True, down)
        return tuple(one for kind in range(3) for one in (*side[2 * kind : 2 * kind + 2], down[kind]))

    return jax.shard_map(
        step,
        mesh=mesh,
        in_specs=(P(("rep", "dp"), None, None),) * 2 + (P(None, None, None),) * 9,
        out_specs=(P("rep", None, None),) * 9,
        check_vma=False,
    )
```

```python
import functools

import jax
import jax.numpy as jnp
from jax import lax
from jax.experimental import pallas as pl
from jax.experimental.pallas import tpu as pltpu
from jax.sharding import PartitionSpec as P


F32, BF16 = jnp.float32, jnp.bfloat16
PARAMS = functools.partial(pltpu.CompilerParams, vmem_limit_bytes=60 * 2**20)


def mm(a, b, ca=1, cb=0):
    return lax.dot_general(a, b, (((ca,), (cb,)), ((), ())), preferred_element_type=F32)


def normed(wide):
    scale = lax.rsqrt(jnp.mean(wide * wide, -1, keepdims=True) + 1e-6)
    return (wide * scale).astype(BF16)


def sigmoid(x):
    return 0.5 * jnp.tanh(0.5 * x) + 0.5


def cost(flops, nbytes):
    return pl.CostEstimate(flops=int(flops), bytes_accessed=int(nbytes), transcendentals=0)


def whole(shape):
    return pl.BlockSpec(shape, lambda *_: (0,) * len(shape), pipeline_mode=pl.Buffered(1))


def layer_of(array, number):
    return pl.BlockSpec((None, *array.shape[1:]), lambda *_: (number, 0, 0), pipeline_mode=pl.Buffered(1))


def chunks(ff, width):
    return [slice(i, i + width) for i in range(0, ff, width)]


def forward_kernel(width, h_ref, wg_ref, wu_ref, wd_ref, o_ref, gate_ref, up_ref, hid_ref):
    wide = h_ref[...].astype(F32)
    a = normed(wide)
    for c in chunks(wg_ref.shape[1], width):
        gate, up = mm(a, wg_ref[:, c]), mm(a, wu_ref[:, c])
        gate_ref[:, c], up_ref[:, c] = gate, up
        hid_ref[:, c] = (gate * sigmoid(gate) * up).astype(BF16)
    y = mm(hid_ref[...], wd_ref[...]).astype(BF16).astype(F32)
    o_ref[...] = (wide + y).astype(BF16)


def forward(number, h, wg, wu, wd, tile=256, width=768):
    tokens, d = h.shape
    ff = wg.shape[2]
    return pl.pallas_call(
        functools.partial(forward_kernel, width),
        name="forward",
        grid=(tokens // tile,),
        in_specs=[pl.BlockSpec((tile, d), lambda i: (i, 0)), layer_of(wg, number), layer_of(wu, number), layer_of(wd, number)],
        out_specs=[pl.BlockSpec((tile, width), lambda i: (i, 0)) for width in (d, ff, ff)],
        out_shape=[jax.ShapeDtypeStruct((tokens, d), BF16)] + [jax.ShapeDtypeStruct((tokens, ff), F32)] * 2,
        scratch_shapes=[pltpu.VMEM((tile, ff), BF16)],
        compiler_params=PARAMS(),
        cost_estimate=cost(6 * tokens * d * ff, 2 * (2 * tokens * d + 3 * d * ff + 4 * tokens * ff)),
    )(h, wg, wu, wd)


PAIRED, PASSED, ARRIVED = 3, 6, 12


def gradients_kernel(size, tile, known, h_ref, dy_ref, gate_ref, up_ref, wd_ref, oa_ref, ob_ref, *refs):
    *kept, a, dy, x, y, g, pr, p, r1a, r1b, r2a, r2b, send, recv, load = refs
    tokens = h_ref.shape[0]
    step = pl.program_id(0)
    steps = pl.num_programs(0) - pl.cdiv(ARRIVED, 3)
    pieces = 3 * steps
    slots = g.shape[0]
    rows = g.shape[1] // size
    width = g.shape[2]
    a_half, b_half = pl.ds(0, width // 2), pl.ds(width // 2, width // 2)
    quarters = size // 2
    me = lax.axis_index("dp")
    core, chip = lax.rem(me, 2), me // 2
    partner = me + 1 - 2 * core
    right, left = lax.rem(me + 2, size), lax.rem(me + size - 2, size)

    def inputs(i):
        t = pl.ds(i, tile)
        pairs = enumerate(((h_ref, a), (dy_ref, dy)))
        return [pltpu.make_async_copy(source.at[t], target.at[t], load.at[which, i // tile]) for which, (source, target) in pairs]

    def of_chip(offset):
        return pl.ds(pl.multiple_of(lax.rem(chip + offset, quarters) * rows, 16), rows)

    def half(which):
        return pl.ds(pl.multiple_of(which * quarters * rows, 16), quarters * rows)

    def copy(kind, j, source, target, device):
        return pltpu.make_async_remote_copy(
            src_ref=source,
            dst_ref=target.at[j],
            send_sem=send.at[kind, j],
            recv_sem=recv.at[kind, j],
            device_id={"dp": device},
            device_id_type=pl.DeviceIdType.MESH,
        )

    def to_partner(j):
        return copy(0, j, g.at[lax.rem(j, slots), half(1 - core)], pr, partner)

    def first(j):
        opposite = of_chip(2)
        return copy(1, j, p.at[j, opposite, a_half], r1a, right), copy(2, j, p.at[j, opposite, b_half], r1b, left)

    def second(j):
        return copy(3, j, p.at[j, of_chip(1)], r2a, right), copy(4, j, p.at[j, of_chip(quarters - 1)], r2b, left)

    @pl.when(step == 0)
    def _():
        for i in range(0, tokens, tile):
            for one in inputs(i):
                one.start()
        barrier = pltpu.get_barrier_semaphore()
        for device in (partner, left, right):
            pl.semaphore_signal(barrier, inc=1, device_id={"dp": device}, device_id_type=pl.DeviceIdType.MESH)
        pl.semaphore_wait(barrier, 3)
        for i in range(0, tokens, tile):
            for one in inputs(i):
                one.wait()
            part = normed(a[i : i + tile].astype(F32))
            a[i : i + tile] = part
            x[0, :, i : i + tile] = dy[i : i + tile].T
            x[1, :, i : i + tile] = part.T

    @pl.when(step < steps)
    def _():
        for i in range(0, tokens, tile):
            t = slice(i, i + tile)
            gate, up = (gate_ref[t], up_ref[t]) if known else (mm(a[t], gate_ref[...]), mm(a[t], up_ref[...]))
            by_hid = mm(dy[t], wd_ref[...], 1, 1).astype(BF16).astype(F32)
            s = sigmoid(gate)
            silu = gate * s
            y[0, t] = (silu * up).astype(BF16)
            dg = (by_hid * up * (s + silu * (1.0 - s))).astype(BF16)
            du = (by_hid * silu).astype(BF16)
            y[1, t] = dg
            y[2, t] = du
            if kept:
                kept[0][0, t] = dg
                kept[0][1, t] = du
        for which in range(3):
            g[lax.rem(3 * step + which, slots)] = mm(x[min(which, 1)], y[which]).astype(BF16)

    @pl.loop(0, 3)
    def _(which):
        k = 3 * step + which

        def stage(after):
            return pl.when((k >= after) & (k < pieces + after))

        @stage(PAIRED)
        def _():
            j = k - PAIRED
            to_partner(j).wait()
            p[j] = (g[lax.rem(j, slots), half(core)].astype(F32) + pr[j].astype(F32)).astype(BF16)

        @stage(PASSED)
        def _():
            j = k - PASSED
            for one in first(j):
                one.wait()
            p[j, of_chip(1), a_half] = (p[j, of_chip(1), a_half].astype(F32) + r1a[j].astype(F32)).astype(BF16)
            p[j, of_chip(quarters - 1), b_half] = (p[j, of_chip(quarters - 1), b_half].astype(F32) + r1b[j].astype(F32)).astype(BF16)

        @stage(ARRIVED)
        def _():
            j = k - ARRIVED
            for one in second(j):
                one.wait()
            total = (p[j, of_chip(0)].astype(F32) + r2a[j].astype(F32) + r2b[j].astype(F32)).astype(BF16)
            for o_ref, first_step in ((oa_ref, 0), (ob_ref, steps // 2)):
                here = (j // 3 - first_step) * width

                @pl.when((here >= 0) & (here < o_ref.shape[2]))
                def _(o_ref=o_ref, here=here):
                    o_ref[lax.rem(j + 2, 3), :, pl.ds(pl.multiple_of(here, 128), width)] = total

        @stage(0)
        def _():
            to_partner(k).start()

        @stage(PAIRED)
        def _():
            for one in first(k - PAIRED):
                one.start()

        @stage(PASSED)
        def _():
            for one in second(k - PASSED):
                one.start()


def gradients(size, number, h, dy, known, wg, wu, wd, keep, width=256, tile=512):
    tokens, d = h.shape
    ff = wg.shape[2]
    tile = tile // 2 if known else tile
    steps, rows, half = ff // width, d // size, d // 2
    pieces = 3 * steps

    def now(k):
        return jnp.minimum(k, steps - 1)

    if known:
        column, pair = pl.BlockSpec((tokens, width), lambda k: (0, now(k))), known
    else:
        column, pair = pl.BlockSpec((None, d, width), lambda k: (number, 0, now(k))), (wg, wu)
    parts = [(3, rows, count * width) for count in (steps // 2, steps - steps // 2)]
    out_specs, out_shape = [whole(one) for one in parts], [jax.ShapeDtypeStruct(one, BF16) for one in parts]
    if keep:
        out_specs += [pl.BlockSpec((2, tokens, width), lambda k: (0, 0, now(k)))]
        out_shape += [jax.ShapeDtypeStruct((2, tokens, ff), BF16)]
    return pl.pallas_call(
        functools.partial(gradients_kernel, size, tile, bool(known)),
        name="gradients",
        grid=(steps + pl.cdiv(ARRIVED, 3),),
        in_specs=[pl.BlockSpec(memory_space=pltpu.HBM)] * 2 + [column, column, pl.BlockSpec((None, width, d), lambda k: (number, now(k), 0))],
        out_specs=out_specs,
        out_shape=out_shape,
        scratch_shapes=[
            pltpu.VMEM((tokens, d), BF16),
            pltpu.VMEM((tokens, d), BF16),
            pltpu.VMEM((2, d, tokens), BF16),
            pltpu.VMEM((3, tokens, width), BF16),
            pltpu.VMEM((PAIRED + 3, d, width), BF16),
            pltpu.VMEM((pieces, half, width), BF16),
            pltpu.VMEM((pieces, half, width), BF16),
            pltpu.VMEM((pieces, rows, width // 2), BF16),
            pltpu.VMEM((pieces, rows, width // 2), BF16),
            pltpu.VMEM((pieces, rows, width), BF16),
            pltpu.VMEM((pieces, rows, width), BF16),
            pltpu.SemaphoreType.DMA((5, pieces)),
            pltpu.SemaphoreType.DMA((5, pieces)),
            pltpu.SemaphoreType.DMA((2, tokens // tile)),
        ],
        compiler_params=PARAMS(collective_id=number, has_side_effects=True),
        cost_estimate=cost((8 if known else 12) * tokens * d * ff, 2 * (2 * tokens * d + 2 * tokens * ff + 6 * d * ff)),
    )(h, dy, *pair, wd)


def back_kernel(h_ref, dy_ref, dg_ref, du_ref, wg_ref, wu_ref, o_ref):
    by_a = mm(dg_ref[...], wg_ref[...], 1, 1).astype(BF16).astype(F32)
    by_a = (by_a + mm(du_ref[...], wu_ref[...], 1, 1).astype(BF16).astype(F32)).astype(BF16).astype(F32)
    wide = h_ref[...].astype(F32)
    scale = lax.rsqrt(jnp.mean(wide * wide, -1, keepdims=True) + 1e-6)
    by_h = scale * by_a - wide * (scale * scale * scale * jnp.mean(by_a * wide, -1, keepdims=True))
    o_ref[...] = (dy_ref[...].astype(F32) + by_h.astype(BF16).astype(F32)).astype(BF16)


def back(number, h, dy, y, wg, wu, tile=256):
    tokens, d = h.shape
    ff = wg.shape[2]
    row = pl.BlockSpec((tile, d), lambda i: (i, 0))
    by_gate, by_up = (pl.BlockSpec((None, tile, ff), lambda i, which=which: (which, i, 0)) for which in (0, 1))
    return pl.pallas_call(
        back_kernel,
        name="back",
        grid=(tokens // tile,),
        in_specs=[row, row, by_gate, by_up, layer_of(wg, number), layer_of(wu, number)],
        out_specs=row,
        out_shape=jax.ShapeDtypeStruct((tokens, d), BF16),
        compiler_params=PARAMS(),
        cost_estimate=cost(4 * tokens * d * ff, 2 * (3 * tokens * d + 2 * d * ff + 2 * tokens * ff)),
    )(h, dy, y, y, wg, wu)


FLIGHT = 4


def adamw_kernel(number, first, count, blocks, size, turned, aliased, *refs):
    parts, refs = refs[:16], refs[16:]
    sources, refs = refs[: 3 * count], refs[3 * count + aliased :]
    targets, refs = refs[: 3 * count], refs[3 * count :]
    g_buf, wi, mi, vi, wo, mo, vo, g_sem, in_sem, out_sem = refs
    rows, per = wi.shape[1], blocks // count
    shard = parts[0].shape[1]
    middle, rest = parts[0].shape[2], parts[1].shape[2]
    quarters = size // 2
    me = lax.axis_index("dp")
    core, chip = lax.rem(me, 2), me // 2

    def place(which):
        at = lax.rem(which, 4)
        offset = jnp.where(at == 1, quarters - 1, jnp.where(at == 2, 1, jnp.where(at == 3, 2, 0)))
        side = jnp.where(which < 4, core, 1 - core)
        return side * quarters + lax.rem(chip + offset, quarters)

    def of_shard(which, matrix, target, sem):
        a, b = parts[2 * which : 2 * which + 2]
        return [
            pltpu.make_async_copy(a.at[matrix], target.at[:, pl.ds(0, middle)], sem),
            pltpu.make_async_copy(b.at[matrix], target.at[:, pl.ds(middle, rest)], sem),
        ]

    def arrived(target, sem):
        pltpu.make_async_copy(target, target, sem).wait()

    def move(c, arrays, buffers, sem, into):
        slot, block = lax.rem(c, FLIGHT), lax.rem(c, per)
        start = block if turned else place(block)
        here = pl.ds(pl.multiple_of(start * rows, 16), rows)
        for matrix in range(count):

            @pl.when(c // per == matrix)
            def _(matrix=matrix):
                for kind in range(3):
                    far, near = arrays[kind * count + matrix].at[number, here], buffers[kind].at[slot]
                    pltpu.make_async_copy(*((far, near) if into else (near, far)), sem.at[kind, slot]).start()

                if into and not turned:
                    for which in range(8):

                        @pl.when(block == which)
                        def _(which=which):
                            for one in of_shard(which, first + matrix, g_buf.at[slot], g_sem.at[slot]):
                                one.start()

    def settle(c, arrays, buffers, sem, into):
        slot = lax.rem(c, FLIGHT)
        for kind in range(3):
            far, near = arrays[kind * count].at[number, pl.ds(0, rows)], buffers[kind].at[slot]
            pltpu.make_async_copy(*((far, near) if into else (near, far)), sem.at[kind, slot]).wait()
        if into and not turned:
            arrived(g_buf.at[slot], g_sem.at[slot])

    def fetch(c):
        move(c, sources, (wi, mi, vi), in_sem, True)

    if turned:
        for which in range(8):
            for one in of_shard(which, first, g_buf.at[pl.ds(pl.multiple_of(place(which) * shard, 16), shard)], g_sem.at[which]):
                one.start()
    for c in range(FLIGHT):
        fetch(c)
    if turned:
        for which in range(8):
            arrived(g_buf.at[pl.ds(0, shard)], g_sem.at[which])

    @pl.loop(0, blocks)
    def _(c):
        slot = lax.rem(c, FLIGHT)
        settle(c, sources, (wi, mi, vi), in_sem, True)

        @pl.when(c >= FLIGHT)
        def _():
            settle(c - FLIGHT, targets, (wo, mo, vo), out_sem, False)

        g = g_buf[:, pl.ds(pl.multiple_of(c * rows, 128), rows)].T if turned else g_buf[slot]
        g = g.astype(F32)
        m = 0.9 * mi[slot] + 0.1 * g
        v = 0.95 * vi[slot] + 0.05 * g * g
        w = wi[slot].astype(F32)
        wo[slot] = (w - 0.02 * (m * lax.rsqrt(v + 1e-8) + 0.1 * w)).astype(BF16)
        mo[slot] = m
        vo[slot] = v
        move(c, targets, (wo, mo, vo), out_sem, False)

        @pl.when(c + FLIGHT < blocks)
        def _():
            fetch(c + FLIGHT)

    for c in range(blocks - FLIGHT, blocks):
        settle(c, targets, (wo, mo, vo), out_sem, False)


def adamw(size, number, first, parts, weights, moments, squares, turned, so_far, width=256):
    count = len(weights)
    shard, ff = parts[0].shape[1], parts[0].shape[2] + parts[1].shape[2]
    d = shard * size
    so_far = so_far or ()
    rows, columns = (width, d) if turned else (shard, ff)
    blocks = count * weights[0].shape[1] // rows
    hbm = pl.BlockSpec(memory_space=pltpu.HBM)
    inputs = (*parts, *weights, *moments, *squares, *so_far)
    return pl.pallas_call(
        functools.partial(adamw_kernel, number, first, count, blocks, size, turned, len(so_far)),
        name="adamw",
        in_specs=[hbm] * len(inputs),
        out_specs=[hbm] * (3 * count),
        out_shape=[jax.ShapeDtypeStruct(one.shape, one.dtype) for one in (*weights, *moments, *squares)],
        scratch_shapes=[
            pltpu.VMEM((d, ff) if turned else (FLIGHT, rows, columns), BF16),
            *[pltpu.VMEM((FLIGHT, rows, columns), dtype) for dtype in (BF16, F32, F32) * 2],
            pltpu.SemaphoreType.DMA((8,) if turned else (FLIGHT,)),
            pltpu.SemaphoreType.DMA((3, FLIGHT)),
            pltpu.SemaphoreType.DMA((3, FLIGHT)),
        ],
        input_output_aliases={16 + 3 * count + i: i for i in range(len(so_far))},
        compiler_params=PARAMS(),
        cost_estimate=cost(count * 5 * 2048 * d * ff // 2, count * 22 * d * ff),
    )(*inputs)


def solution(mesh):
    size = mesh.shape["dp"]
    swap = [(i, i ^ 1) for i in range(size)]
    to_right = [(i, (i + 2) % size) for i in range(size)]
    to_left = [(i, (i - 2) % size) for i in range(size)]

    def step(x, dy, *arrays):
        weights, moments, squares = (arrays[i : i + 3] for i in (0, 3, 6))
        layers = weights[0].shape[0]

        def hop(one, to):
            return lax.ppermute(one, "dp", to)

        def gathered(a, b):
            near, far, last = (hop for _ in range(3))
            mine = [a, b, near(a, to_right), near(b, to_right), near(a, to_left), near(b, to_left)]
            mine += [far(mine[2], to_right), far(mine[5], to_left)]
            hops = (near, near, far, far, far, far, last, last)
            return (*mine, *(by(one, swap) for by, one in zip(hops, mine, strict=True)))

        h, kept, known = x[0], [], []
        for number in range(layers):
            kept.append(h)
            both = ()
            if number < layers - 1:
                h, *both = forward(number, h, *weights)
            known.append(both)
        by_h, every = dy[0], []
        for number in reversed(range(layers)):
            a, b, *by_both = gradients(size, number, kept[number], by_h, known[number], *weights, number > 0)
            every.append((number, gathered(a, b)))
            if number:
                by_h = back(number, kept[number], by_h, by_both[0], *weights[:2])
        side, down = None, None
        for number, parts in every:
            side = adamw(size, number, 0, parts, weights[:2], moments[:2], squares[:2], False, side)
            down = adamw(size, number, 2, parts, weights[2:], moments[2:], squares[2:], True, down)
        return tuple(one for kind in range(3) for one in (*side[2 * kind : 2 * kind + 2], down[kind]))

    return jax.shard_map(
        step,
        mesh=mesh,
        in_specs=(P(("rep", "dp"), None, None),) * 2 + (P(None, None, None),) * 9,
        out_specs=(P("rep", None, None),) * 9,
        check_vma=False,
    )
```

```python
import functools

import jax
import jax.numpy as jnp
from jax import lax
from jax.experimental import pallas as pl
from jax.experimental.pallas import tpu as pltpu
from jax.sharding import PartitionSpec as P


F32, BF16 = jnp.float32, jnp.bfloat16
PARAMS = functools.partial(pltpu.CompilerParams, vmem_limit_bytes=60 * 2**20)


def mm(a, b, ca=1, cb=0):
    return lax.dot_general(a, b, (((ca,), (cb,)), ((), ())), preferred_element_type=F32)


def normed(wide):
    scale = lax.rsqrt(jnp.mean(wide * wide, -1, keepdims=True) + 1e-6)
    return (wide * scale).astype(BF16)


def sigmoid(x):
    return 0.5 * jnp.tanh(0.5 * x) + 0.5


def cost(flops, nbytes):
    return pl.CostEstimate(flops=int(flops), bytes_accessed=int(nbytes), transcendentals=0)


def whole(shape):
    return pl.BlockSpec(shape, lambda *_: (0,) * len(shape), pipeline_mode=pl.Buffered(1))


def layer_of(array, number):
    return pl.BlockSpec((None, *array.shape[1:]), lambda *_: (number, 0, 0), pipeline_mode=pl.Buffered(1))


def chunks(ff, width):
    return [slice(i, i + width) for i in range(0, ff, width)]


def forward_kernel(width, h_ref, wg_ref, wu_ref, wd_ref, o_ref, gate_ref, up_ref, hid_ref):
    wide = h_ref[...].astype(F32)
    a = normed(wide)
    for c in chunks(wg_ref.shape[1], width):
        gate, up = mm(a, wg_ref[:, c]), mm(a, wu_ref[:, c])
        gate_ref[:, c], up_ref[:, c] = gate, up
        hid_ref[:, c] = (gate * sigmoid(gate) * up).astype(BF16)
    y = mm(hid_ref[...], wd_ref[...]).astype(BF16).astype(F32)
    o_ref[...] = (wide + y).astype(BF16)


def forward(number, h, wg, wu, wd, tile=512, width=256):
    tokens, d = h.shape
    ff = wg.shape[2]
    return pl.pallas_call(
        functools.partial(forward_kernel, width),
        name="forward",
        grid=(tokens // tile,),
        in_specs=[pl.BlockSpec((tile, d), lambda i: (i, 0)), layer_of(wg, number), layer_of(wu, number), layer_of(wd, number)],
        out_specs=[pl.BlockSpec((tile, width), lambda i: (i, 0)) for width in (d, ff, ff)],
        out_shape=[jax.ShapeDtypeStruct((tokens, d), BF16)] + [jax.ShapeDtypeStruct((tokens, ff), F32)] * 2,
        scratch_shapes=[pltpu.VMEM((tile, ff), BF16)],
        compiler_params=PARAMS(),
        cost_estimate=cost(6 * tokens * d * ff, 2 * (2 * tokens * d + 3 * d * ff + 4 * tokens * ff)),
    )(h, wg, wu, wd)


PAIRED, PASSED, ARRIVED = 3, 6, 12


def gradients_kernel(size, tile, known, h_ref, dy_ref, gate_ref, up_ref, wd_ref, oa_ref, ob_ref, *refs):
    *kept, a, dy, x, y, g, pr, p, r1a, r1b, r2a, r2b, send, recv, load = refs
    tokens = h_ref.shape[0]
    step = pl.program_id(0)
    steps = pl.num_programs(0) - pl.cdiv(ARRIVED, 3)
    pieces = 3 * steps
    slots = g.shape[0]
    rows = g.shape[1] // size
    width = g.shape[2]
    a_half, b_half = pl.ds(0, width // 2), pl.ds(width // 2, width // 2)
    quarters = size // 2
    me = lax.axis_index("dp")
    core, chip = lax.rem(me, 2), me // 2
    partner = me + 1 - 2 * core
    right, left = lax.rem(me + 2, size), lax.rem(me + size - 2, size)

    def inputs(i):
        t = pl.ds(i, tile)
        pairs = enumerate(((h_ref, a), (dy_ref, dy)))
        return [pltpu.make_async_copy(source.at[t], target.at[t], load.at[which, i // tile]) for which, (source, target) in pairs]

    def of_chip(offset):
        return pl.ds(pl.multiple_of(lax.rem(chip + offset, quarters) * rows, 16), rows)

    def half(which):
        return pl.ds(pl.multiple_of(which * quarters * rows, 16), quarters * rows)

    def copy(kind, j, source, target, device):
        return pltpu.make_async_remote_copy(
            src_ref=source,
            dst_ref=target.at[j],
            send_sem=send.at[kind, j],
            recv_sem=recv.at[kind, j],
            device_id={"dp": device},
            device_id_type=pl.DeviceIdType.MESH,
        )

    def to_partner(j):
        return copy(0, j, g.at[lax.rem(j, slots), half(1 - core)], pr, partner)

    def first(j):
        opposite = of_chip(2)
        return copy(1, j, p.at[j, opposite, a_half], r1a, right), copy(2, j, p.at[j, opposite, b_half], r1b, left)

    def second(j):
        return copy(3, j, p.at[j, of_chip(1)], r2a, right), copy(4, j, p.at[j, of_chip(quarters - 1)], r2b, left)

    @pl.when(step == 0)
    def _():
        for i in range(0, tokens, tile):
            for one in inputs(i):
                one.start()
        barrier = pltpu.get_barrier_semaphore()
        for device in (partner, left, right):
            pl.semaphore_signal(barrier, inc=1, device_id={"dp": device}, device_id_type=pl.DeviceIdType.MESH)
        pl.semaphore_wait(barrier, 3)
        for i in range(0, tokens, tile):
            for one in inputs(i):
                one.wait()
            part = normed(a[i : i + tile].astype(F32))
            a[i : i + tile] = part
            x[0, :, i : i + tile] = dy[i : i + tile].T
            x[1, :, i : i + tile] = part.T

    @pl.when(step < steps)
    def _():
        for i in range(0, tokens, tile):
            t = slice(i, i + tile)
            gate, up = (gate_ref[t], up_ref[t]) if known else (mm(a[t], gate_ref[...]), mm(a[t], up_ref[...]))
            by_hid = mm(dy[t], wd_ref[...], 1, 1).astype(BF16).astype(F32)
            s = sigmoid(gate)
            silu = gate * s
            y[0, t] = (silu * up).astype(BF16)
            dg = (by_hid * up * (s + silu * (1.0 - s))).astype(BF16)
            du = (by_hid * silu).astype(BF16)
            y[1, t] = dg
            y[2, t] = du
            if kept:
                kept[0][0, t] = dg
                kept[0][1, t] = du
        for which in range(3):
            g[lax.rem(3 * step + which, slots)] = mm(x[min(which, 1)], y[which]).astype(BF16)

    @pl.loop(0, 3)
    def _(which):
        k = 3 * step + which

        def stage(after):
            return pl.when((k >= after) & (k < pieces + after))

        @stage(PAIRED)
        def _():
            j = k - PAIRED
            to_partner(j).wait()
            p[j] = (g[lax.rem(j, slots), half(core)].astype(F32) + pr[j].astype(F32)).astype(BF16)

        @stage(PASSED)
        def _():
            j = k - PASSED
            for one in first(j):
                one.wait()
            p[j, of_chip(1), a_half] = (p[j, of_chip(1), a_half].astype(F32) + r1a[j].astype(F32)).astype(BF16)
            p[j, of_chip(quarters - 1), b_half] = (p[j, of_chip(quarters - 1), b_half].astype(F32) + r1b[j].astype(F32)).astype(BF16)

        @stage(ARRIVED)
        def _():
            j = k - ARRIVED
            for one in second(j):
                one.wait()
            total = (p[j, of_chip(0)].astype(F32) + r2a[j].astype(F32) + r2b[j].astype(F32)).astype(BF16)
            for o_ref, first_step in ((oa_ref, 0), (ob_ref, steps // 2)):
                here = (j // 3 - first_step) * width

                @pl.when((here >= 0) & (here < o_ref.shape[2]))
                def _(o_ref=o_ref, here=here):
                    o_ref[lax.rem(j + 2, 3), :, pl.ds(pl.multiple_of(here, 128), width)] = total

        @stage(0)
        def _():
            to_partner(k).start()

        @stage(PAIRED)
        def _():
            for one in first(k - PAIRED):
                one.start()

        @stage(PASSED)
        def _():
            for one in second(k - PASSED):
                one.start()


def gradients(size, number, h, dy, known, wg, wu, wd, keep, width=256, tile=1024):
    tokens, d = h.shape
    ff = wg.shape[2]
    tile = tile // 2 if known else tile
    steps, rows, half = ff // width, d // size, d // 2
    pieces = 3 * steps

    def now(k):
        return jnp.minimum(k, steps - 1)

    if known:
        column, pair = pl.BlockSpec((tokens, width), lambda k: (0, now(k))), known
    else:
        column, pair = pl.BlockSpec((None, d, width), lambda k: (number, 0, now(k))), (wg, wu)
    parts = [(3, rows, count * width) for count in (steps // 2, steps - steps // 2)]
    out_specs, out_shape = [whole(one) for one in parts], [jax.ShapeDtypeStruct(one, BF16) for one in parts]
    if keep:
        out_specs += [pl.BlockSpec((2, tokens, width), lambda k: (0, 0, now(k)))]
        out_shape += [jax.ShapeDtypeStruct((2, tokens, ff), BF16)]
    return pl.pallas_call(
        functools.partial(gradients_kernel, size, tile, bool(known)),
        name="gradients",
        grid=(steps + pl.cdiv(ARRIVED, 3),),
        in_specs=[pl.BlockSpec(memory_space=pltpu.HBM)] * 2 + [column, column, pl.BlockSpec((None, width, d), lambda k: (number, now(k), 0))],
        out_specs=out_specs,
        out_shape=out_shape,
        scratch_shapes=[
            pltpu.VMEM((tokens, d), BF16),
            pltpu.VMEM((tokens, d), BF16),
            pltpu.VMEM((2, d, tokens), BF16),
            pltpu.VMEM((3, tokens, width), BF16),
            pltpu.VMEM((PAIRED + 3, d, width), BF16),
            pltpu.VMEM((pieces, half, width), BF16),
            pltpu.VMEM((pieces, half, width), BF16),
            pltpu.VMEM((pieces, rows, width // 2), BF16),
            pltpu.VMEM((pieces, rows, width // 2), BF16),
            pltpu.VMEM((pieces, rows, width), BF16),
            pltpu.VMEM((pieces, rows, width), BF16),
            pltpu.SemaphoreType.DMA((5, pieces)),
            pltpu.SemaphoreType.DMA((5, pieces)),
            pltpu.SemaphoreType.DMA((2, tokens // tile)),
        ],
        compiler_params=PARAMS(collective_id=number, has_side_effects=True),
        cost_estimate=cost((8 if known else 12) * tokens * d * ff, 2 * (2 * tokens * d + 2 * tokens * ff + 6 * d * ff)),
    )(h, dy, *pair, wd)


def back_kernel(h_ref, dy_ref, dg_ref, du_ref, wg_ref, wu_ref, o_ref):
    by_a = mm(dg_ref[...], wg_ref[...], 1, 1).astype(BF16).astype(F32)
    by_a = (by_a + mm(du_ref[...], wu_ref[...], 1, 1).astype(BF16).astype(F32)).astype(BF16).astype(F32)
    wide = h_ref[...].astype(F32)
    scale = lax.rsqrt(jnp.mean(wide * wide, -1, keepdims=True) + 1e-6)
    by_h = scale * by_a - wide * (scale * scale * scale * jnp.mean(by_a * wide, -1, keepdims=True))
    o_ref[...] = (dy_ref[...].astype(F32) + by_h.astype(BF16).astype(F32)).astype(BF16)


def back(number, h, dy, y, wg, wu, tile=256):
    tokens, d = h.shape
    ff = wg.shape[2]
    row = pl.BlockSpec((tile, d), lambda i: (i, 0))
    by_gate, by_up = (pl.BlockSpec((None, tile, ff), lambda i, which=which: (which, i, 0)) for which in (0, 1))
    return pl.pallas_call(
        back_kernel,
        name="back",
        grid=(tokens // tile,),
        in_specs=[row, row, by_gate, by_up, layer_of(wg, number), layer_of(wu, number)],
        out_specs=row,
        out_shape=jax.ShapeDtypeStruct((tokens, d), BF16),
        compiler_params=PARAMS(),
        cost_estimate=cost(4 * tokens * d * ff, 2 * (3 * tokens * d + 2 * d * ff + 2 * tokens * ff)),
    )(h, dy, y, y, wg, wu)


FLIGHT = 4


def adamw_kernel(number, first, count, blocks, begin, size, turned, aliased, *refs):
    parts, refs = refs[:16], refs[16:]
    sources, refs = refs[: 3 * count], refs[3 * count + aliased :]
    targets, refs = refs[: 3 * count], refs[3 * count :]
    g_buf, wi, mi, vi, wo, mo, vo, g_sem, in_sem, out_sem = refs
    rows, per, flight = wi.shape[1], blocks // count, wi.shape[0]
    shard = parts[0].shape[1]
    middle, rest = parts[0].shape[2], parts[1].shape[2]
    quarters = size // 2
    me = lax.axis_index("dp")
    core, chip = lax.rem(me, 2), me // 2

    def place(which):
        at = lax.rem(which, 4)
        offset = jnp.where(at == 1, quarters - 1, jnp.where(at == 2, 1, jnp.where(at == 3, 2, 0)))
        side = jnp.where(which < 4, core, 1 - core)
        return side * quarters + lax.rem(chip + offset, quarters)

    def of_shard(which, matrix, target, sem):
        a, b = parts[2 * which : 2 * which + 2]
        return [
            pltpu.make_async_copy(a.at[matrix], target.at[:, pl.ds(0, middle)], sem),
            pltpu.make_async_copy(b.at[matrix], target.at[:, pl.ds(middle, rest)], sem),
        ]

    def arrived(target, sem):
        pltpu.make_async_copy(target, target, sem).wait()

    def move(c, arrays, buffers, sem, into):
        slot, block = lax.rem(c, flight), begin + lax.rem(c, per)
        start = block if turned else place(block)
        here = pl.ds(pl.multiple_of(start * rows, 16), rows)
        for matrix in range(count):

            @pl.when(c // per == matrix)
            def _(matrix=matrix):
                for kind in range(3):
                    far, near = arrays[kind * count + matrix].at[number, here], buffers[kind].at[slot]
                    pltpu.make_async_copy(*((far, near) if into else (near, far)), sem.at[kind, slot]).start()

                if into and not turned:
                    for which in range(begin, begin + per):

                        @pl.when(block == which)
                        def _(which=which):
                            for one in of_shard(which, first + matrix, g_buf.at[slot], g_sem.at[slot]):
                                one.start()

    def settle(c, arrays, buffers, sem, into):
        slot = lax.rem(c, flight)
        for kind in range(3):
            far, near = arrays[kind * count].at[number, pl.ds(0, rows)], buffers[kind].at[slot]
            pltpu.make_async_copy(*((far, near) if into else (near, far)), sem.at[kind, slot]).wait()
        if into and not turned:
            arrived(g_buf.at[slot], g_sem.at[slot])

    def fetch(c):
        move(c, sources, (wi, mi, vi), in_sem, True)

    if turned:
        for which in range(8):
            for one in of_shard(which, first, g_buf.at[pl.ds(pl.multiple_of(place(which) * shard, 16), shard)], g_sem.at[which]):
                one.start()
    for c in range(flight):
        fetch(c)
    if turned:
        for which in range(8):
            arrived(g_buf.at[pl.ds(0, shard)], g_sem.at[which])

    @pl.loop(0, blocks)
    def _(c):
        slot = lax.rem(c, flight)
        settle(c, sources, (wi, mi, vi), in_sem, True)

        @pl.when(c >= flight)
        def _():
            settle(c - flight, targets, (wo, mo, vo), out_sem, False)

        g = g_buf[:, pl.ds(pl.multiple_of(c * rows, 128), rows)].T if turned else g_buf[slot]
        g = g.astype(F32)
        m = 0.9 * mi[slot] + 0.1 * g
        v = 0.95 * vi[slot] + 0.05 * g * g
        w = wi[slot].astype(F32)
        wo[slot] = (w - 0.02 * (m * lax.rsqrt(v + 1e-8) + 0.1 * w)).astype(BF16)
        mo[slot] = m
        vo[slot] = v
        move(c, targets, (wo, mo, vo), out_sem, False)

        @pl.when(c + flight < blocks)
        def _():
            fetch(c + flight)

    for c in range(blocks - flight, blocks):
        settle(c, targets, (wo, mo, vo), out_sem, False)


def adamw(size, number, first, parts, weights, moments, squares, turned, so_far, begin=0, end=8, width=256):
    count = len(weights)
    shard, ff = parts[0].shape[1], parts[0].shape[2] + parts[1].shape[2]
    d = shard * size
    so_far = so_far or ()
    rows, columns = (width, d) if turned else (shard, ff)
    blocks = count * (weights[0].shape[1] // rows if turned else end - begin)
    flight = min(FLIGHT, blocks)
    hbm = pl.BlockSpec(memory_space=pltpu.HBM)
    inputs = (*parts, *weights, *moments, *squares, *so_far)
    return pl.pallas_call(
        functools.partial(adamw_kernel, number, first, count, blocks, begin, size, turned, len(so_far)),
        name="adamw",
        in_specs=[hbm] * len(inputs),
        out_specs=[hbm] * (3 * count),
        out_shape=[jax.ShapeDtypeStruct(one.shape, one.dtype) for one in (*weights, *moments, *squares)],
        scratch_shapes=[
            pltpu.VMEM((d, ff) if turned else (flight, rows, columns), BF16),
            *[pltpu.VMEM((flight, rows, columns), dtype) for dtype in (BF16, F32, F32) * 2],
            pltpu.SemaphoreType.DMA((8,) if turned else (flight,)),
            pltpu.SemaphoreType.DMA((3, flight)),
            pltpu.SemaphoreType.DMA((3, flight)),
        ],
        input_output_aliases={16 + 3 * count + i: i for i in range(len(so_far))},
        compiler_params=PARAMS(),
        cost_estimate=cost(count * 5 * 2048 * d * ff // 2, count * 22 * d * ff),
    )(*inputs)


def solution(mesh):
    size = mesh.shape["dp"]
    swap = [(i, i ^ 1) for i in range(size)]
    to_right = [(i, (i + 2) % size) for i in range(size)]
    to_left = [(i, (i - 2) % size) for i in range(size)]

    def step(x, dy, *arrays):
        weights, moments, squares = (arrays[i : i + 3] for i in (0, 3, 6))
        layers = weights[0].shape[0]

        def hop(one, to):
            return lax.ppermute(one, "dp", to)

        def gathered(a, b):
            near, far, last = (hop for _ in range(3))
            mine = [a, b, near(a, to_right), near(b, to_right), near(a, to_left), near(b, to_left)]
            mine += [far(mine[2], to_right), far(mine[5], to_left)]
            hops = (near, near, far, far, far, far, last, last)
            return (*mine, *(by(one, swap) for by, one in zip(hops, mine, strict=True)))

        h, kept, known = x[0], [], []
        for number in range(layers):
            kept.append(h)
            both = ()
            if number < layers - 1:
                h, *both = forward(number, h, *weights)
            known.append(both)
        by_h, every = dy[0], []
        for number in reversed(range(layers)):
            a, b, *by_both = gradients(size, number, kept[number], by_h, known[number], *weights, number > 0)
            every.append((number, gathered(a, b)))
            if number:
                by_h = back(number, kept[number], by_h, by_both[0], *weights[:2])
        side, down = None, None
        for number, parts in every:
            ends = (weights[:2], moments[:2], squares[:2], False)
            if number:
                side = adamw(size, number, 0, parts, *ends, side)
            else:
                side = adamw(size, number, 0, (*parts[:14], *parts[:2]), *ends, side, 0, 7)
                side = adamw(size, number, 0, parts, *ends, side, 7, 8)
            down = adamw(size, number, 2, parts, weights[2:], moments[2:], squares[2:], True, down)
        return tuple(one for kind in range(3) for one in (*side[2 * kind : 2 * kind + 2], down[kind]))

    return jax.shard_map(
        step,
        mesh=mesh,
        in_specs=(P(("rep", "dp"), None, None),) * 2 + (P(None, None, None),) * 9,
        out_specs=(P("rep", None, None),) * 9,
        check_vma=False,
    )
```
